128 devices in a mesh: row: 8 (over z, core), col: 16 (over x, y).
Axes of the slice: x: 4, y: 4, z: 4, core: 2. Of those that a mesh axis runs over, the one named last changes fastest.
Arguments:
- adjacency: int32 [65536, 4096], P('col', 'row'), may hold values from -2147483648 to 2147483647, as said below
- frontier: bfloat16 [131072, 128], P(('row', 'col')), may hold values from 0 to 1, as said below
- visited: int32 [4, 65536], P(None, ('col', 'row')), may hold values from -2147483648 to 2147483647, as said below
Outputs:
- path_counts: float32 [65536, 128], P(('col', 'row'))
- reached_bits: int32 [4, 65536], P(None, ('col', 'row'))
The draws below stay inside these ranges and needn't reach their ends.
Inputs may be any that keep to these rules, and one draw needn't show every extreme that they name: Bit k of adjacency[d, w] is the edge from source vertex 32 w + k to destination d; degrees and edge densities differ between vertices and between blocks of 128 by 128 vertices. `frontier`: values are zero or between 0.1 and 1. Bit k of visited[w, d] tells whether destination d was reached from root 32 w + k.
All inputs are finite; a program needn't handle non-finite values.
Results may differ from the reference program's by a relative error of at most 0.0003.
Values may be sent and summed in bfloat16 or wider, within the bound.
No kernel may reach another device: no remote copies, remote signals or barrier semaphores. Data moves between devices by JAX's collectives and lax.ppermute only.
A program may use at most 64 MiB of HBM per device.

```python
import functools
import math
import jax
import jax.numpy as jnp
from jax import lax

SOURCES = 128
NDST = 65536
NSRC = 131072
WORDS = 4


def draw_adjacency(key, part):
    column_words = NSRC // 32
    key_list = jax.random.split(jax.random.fold_in(key, 11), 6)
    vertex_level = jax.random.randint(key_list[0], (NDST, 1), 0, 8, dtype=jnp.int32)
    tile_level = jax.random.randint(key_list[1], (NDST // 128, column_words // 4), 0, 3, dtype=jnp.int32)
    tile_level = jnp.repeat(jnp.repeat(tile_level, 128, axis=0), 4, axis=1)
    rate_base = jnp.int32(2097152 // NSRC)
    threshold = jnp.left_shift(rate_base, vertex_level + tile_level)
    selector = jax.random.randint(key_list[2], (NDST, column_words), 0, 1048576, dtype=jnp.int32)
    packed_words = jax.random.randint(key_list[3], (NDST, column_words), -2147483648, 2147483647, dtype=jnp.int32)
    for section_index in range(2):
        extra_words = jax.random.randint(key_list[4 + section_index], (NDST, column_words), -2147483648, 2147483647, dtype=jnp.int32)
        packed_words = jnp.bitwise_and(packed_words, extra_words)
    return jnp.where(selector < threshold, packed_words, jnp.int32(0))


def draw_frontier(key, part):
    key_list = jax.random.split(jax.random.fold_in(key, 23), 2)
    keep_mask = jax.random.uniform(key_list[0], (NSRC, SOURCES), jnp.float32) < 0.5
    magnitude = 0.1 * jnp.exp(jax.random.uniform(key_list[1], (NSRC, SOURCES), jnp.float32) * math.log(10.0))
    values = jnp.where(keep_mask, magnitude, jnp.float32(0.0))
    return values.astype(jnp.bfloat16)


def draw_visited(key, part):
    key_list = jax.random.split(jax.random.fold_in(key, 37), 2)
    first_words = jax.random.randint(key_list[0], (WORDS, NDST), -2147483648, 2147483647, dtype=jnp.int32)
    second_words = jax.random.randint(key_list[1], (WORDS, NDST), -2147483648, 2147483647, dtype=jnp.int32)
    return jnp.bitwise_and(first_words, second_words)


def setup_inputs(seed: int = 0) -> dict:
    arg_keys = jax.random.split(jax.random.key(seed), 4)
    return {
        "adjacency": draw_adjacency(jax.random.fold_in(arg_keys[3], 71), 0),
        "frontier": draw_frontier(jax.random.fold_in(arg_keys[3], 71), 0),
        "visited": draw_visited(jax.random.fold_in(arg_keys[3], 71), 0),
    }


def expand_bits(packed):
    shift_table = jnp.arange(32, dtype=jnp.int32)
    bit_table = jnp.bitwise_and(jnp.right_shift(packed[:, :, None], shift_table), 1)
    return bit_table.reshape(packed.shape[0], packed.shape[1] * 32).astype(jnp.bfloat16)


def finish(reached, visited):
    row_count = reached.shape[0]
    word_count = visited.shape[0]
    shift_table = jnp.arange(32, dtype=jnp.int32)
    seen_bits = jnp.bitwise_and(jnp.right_shift(visited[:, :, None], shift_table), 1)
    seen_bits = jnp.transpose(seen_bits, (1, 0, 2)).reshape(row_count, word_count * 32)
    path_counts = jnp.where(seen_bits == 1, jnp.float32(0.0), reached)
    fresh = jnp.logical_and(seen_bits == 0, reached > 0).astype(jnp.int32)
    fresh = fresh.reshape(row_count, word_count, 32)
    added = functools.reduce(jnp.bitwise_or, [jnp.left_shift(fresh[:, :, position], position) for position in range(32)])
    reached_bits = jnp.bitwise_or(visited, jnp.transpose(added))
    return path_counts, reached_bits


def reference(adjacency, frontier, visited):
    dst_total = adjacency.shape[0]
    block_len = math.gcd(dst_total, 512)
    blocks = adjacency.reshape(dst_total // block_len, block_len, adjacency.shape[1])

    def one_block(packed):
        return jnp.dot(expand_bits(packed), frontier, preferred_element_type=jnp.float32)

    reached = lax.map(one_block, blocks).reshape(dst_total, frontier.shape[1])
    return finish(reached, visited)
```

```python
import functools

import jax
import jax.numpy as jnp
import numpy as np
from jax import lax
from jax.experimental import pallas as pl
from jax.experimental.pallas import tpu as pltpu
from jax.sharding import PartitionSpec as P

SIDE = 4
TILE = 256
CHUNK = 1024
TILES = CHUNK // TILE
BITS = 8

VM = pltpu.VMEM
FULL = pl.BlockSpec(memory_space=VM)
SCAL = pl.BlockSpec(memory_space=pltpu.SMEM)

AXES = ("row", "col")


def place(x, y, z, core):
    return (z * 2 + core) * (SIDE * SIDE) + x * SIDE + y


def pairs(axis, flip=False):
    out = []
    for x in range(SIDE):
        for y in range(SIDE):
            for z in range(SIDE):
                for core in range(2):
                    at = [x, y, z]
                    if axis == "core":
                        out.append((place(*at, core), place(*at, 1 - core)))
                        continue
                    n = "xyz".index(axis)
                    step = 1 if (core == 0) != flip else -1
                    to = list(at)
                    to[n] = (to[n] + step) % SIDE
                    out.append((place(*at, core), place(*to, core)))
    return out


def send(value, axis, flip=False):
    return lax.ppermute(value, AXES, pairs(axis, flip))


def swap(value):
    return lax.ppermute(value, AXES, pairs("core"))


def prep_kernel(f_ref, o_ref, s_ref):
    s_ref[...] = f_ref[...].astype(jnp.float32)
    for j in range(TILES):
        rows = []
        for b in range(BITS):
            scale = 2.0**-b if b < 7 else -(2.0**-7)
            rows.append(s_ref[pl.ds(8 * j + b, 32, stride=32), :] * scale)
        o_ref[j] = jnp.concatenate(rows, 0).T.astype(jnp.bfloat16)


def prep(f):
    return pl.pallas_call(
        prep_kernel,
        out_shape=VM((TILES, 128, TILE), jnp.bfloat16),
        in_specs=[FULL],
        out_specs=FULL,
        scratch_shapes=[pltpu.VMEM((CHUNK, 128), jnp.float32)],
        name="prep",
    )(f)


def split_kernel(a_ref, o_ref):
    k = pl.program_id(0)
    i = pl.program_id(1)
    a = a_ref[...]
    for j in range(4):
        part = (lax.shift_right_logical(a, 8 * j) if j else a).astype(jnp.int8).T
        for h in range(2):
            for c in range(4):
                o_ref[2 * k + h, 16 * i + 4 * c + j] = part[32 * c : 32 * c + 32, 512 * h : 512 * h + 512]


def split(adj):
    d, w = adj.shape
    return pl.pallas_call(
        split_kernel,
        grid=(d // 1024, w // 128),
        in_specs=[pl.BlockSpec((1024, 128), lambda k, i: (k, i))],
        out_specs=FULL,
        out_shape=VM((d // 512, w // 8, 32, 512), jnp.int8),
        compiler_params=pltpu.CompilerParams(vmem_limit_bytes=24 << 20),
        name="split",
    )(adj)


def expand(a_ref, r, tiles, at):
    parts = []
    for t in range(tiles):
        x = a_ref[r, at(t)]
        for b in range(BITS):
            m = 1 << b if b < 7 else -128
            parts.append((x & jnp.int8(m)).astype(jnp.bfloat16))
    return jnp.concatenate(parts, 0)


def mm_kernel(*refs, first, group, picks, whole, acc_in):
    idx_ref, a_ref = refs[0], refs[1]
    refs = refs[2:]
    if acc_in:
        acc_ref, refs = refs[0], refs[1:]
    srcs = sorted({p[0] for p in picks})
    f_refs, rest = refs[: len(srcs)], refs[len(srcs) :]
    outs, scr = rest[:-1], rest[-1]
    for t, (n, k) in enumerate(picks):
        scr[t] = f_refs[n][k]
    steps = len(picks) // group

    def step(i, carry):
        base = i * group if steps > 1 else 0
        f = jnp.concatenate([scr[base + t] for t in range(group)], 1)
        at = lambda t: idx_ref[first + base + t]
        if whole:
            out = outs[0]
            for r in range(8):
                got = jnp.dot(f, expand(a_ref, r, group, at), preferred_element_type=jnp.float32)
                out[r] = out[r] + got
        else:
            for n in range(2):
                r = idx_ref[64 + whole_off[0] + n]
                got = jnp.dot(f, expand(a_ref, r, group, at), preferred_element_type=jnp.float32)
                if steps > 1:
                    outs[n][...] += got
                else:
                    outs[n][...] = got + acc_ref[r]
        return carry

    whole_off = (0,)
    if not isinstance(whole, bool):
        whole_off, whole = (whole,), False
    if whole:
        if acc_in:
            outs[0][...] = acc_ref[...]
        else:
            outs[0][...] = jnp.zeros_like(outs[0])
    elif steps > 1:
        for n in range(2):
            outs[n][...] = acc_ref[idx_ref[64 + whole_off[0] + n]]
    if steps > 1:
        lax.fori_loop(0, steps, step, 0)
    else:
        step(0, 0)


def mm(idx, ab, acc, arrays, picks, first, group, whole=True):
    tiles = len(picks)
    if whole is True:
        out_shape = VM((8, 128, 512), jnp.float32)
        out_specs = FULL
        lanes = 4096
    else:
        out_shape = (VM((128, 512), jnp.float32),) * 2
        out_specs = (FULL, FULL)
        lanes = 1024
    args = [idx, ab] + ([acc] if acc is not None else []) + list(arrays)
    alias = {2: 0} if whole is True and acc is not None else {}
    return pl.pallas_call(
        functools.partial(mm_kernel, first=first, group=group, picks=tuple(picks), whole=whole, acc_in=acc is not None),
        out_shape=out_shape,
        in_specs=[SCAL] + [FULL] * (len(args) - 1),
        out_specs=out_specs,
        scratch_shapes=[pltpu.VMEM((tiles, 128, TILE), jnp.bfloat16)],
        input_output_aliases=alias,
        cost_estimate=pl.CostEstimate(flops=2 * 128 * TILE * tiles * lanes, bytes_accessed=0, transcendentals=0),
        compiler_params=pltpu.CompilerParams(vmem_limit_bytes=32 << 20),
        name="bits_mm",
    )(*args)


def finish_kernel(a_ref, b_ref, c_ref, d_ref, v_ref, p_ref, o_ref):
    reached = a_ref[...] + b_ref[...] + c_ref[...] + d_ref[...]
    shift = lax.broadcasted_iota(jnp.int32, (32, 1), 0)
    rows = []
    words = []
    for w in range(4):
        got = reached[32 * w : 32 * w + 32]
        word = v_ref[w : w + 1]
        unseen = (lax.shift_right_arithmetic(jnp.broadcast_to(word, got.shape), jnp.broadcast_to(shift, got.shape)) & 1) == 0
        rows.append(jnp.where(unseen, got, 0.0))
        fresh = jnp.where(unseen & (got > 0), lax.shift_left(jnp.int32(1), jnp.broadcast_to(shift, got.shape)), 0)
        words.append(word | jnp.sum(fresh, 0, keepdims=True))
    p_ref[...] = jnp.concatenate(rows, 0).T
    o_ref[...] = jnp.concatenate(words, 0)


def finish(parts, visited):
    return pl.pallas_call(
        finish_kernel,
        out_shape=(jax.ShapeDtypeStruct((512, 128), jnp.float32), jax.ShapeDtypeStruct((4, 512), jnp.int32)),
        in_specs=[FULL] * 5,
        out_specs=(FULL, FULL),
        name="finish",
    )(*parts, visited)


O, M, Q, T = (0, 0), (-1, 0), (1, 0), (0, 1)


def shards(adjacency, frontier, visited):
    row, col = lax.axis_index("row"), lax.axis_index("col")
    x, y, z, core = col // SIDE, col % SIDE, row // 2, row % 2
    s = 1 - 2 * core

    lists = []

    def tiles(array, start, dx, dy, js):
        return [(array, start + n, dx, dy, j) for n, j in enumerate(js)]

    H0, H1, ALL = (0, 1), (2, 3), (0, 1, 2, 3)
    ph0 = tiles(0, 0, O, O, ALL)
    ph1 = tiles(0, 0, M, O, ALL) + tiles(1, 4, Q, O, ALL) + tiles(2, 0, O, M, ALL) + tiles(3, 4, O, Q, ALL)
    ph2 = (
        tiles(0, 0, T, O, ALL)
        + tiles(1, 0, O, T, ALL)
        + tiles(2, 0, M, M, H1)
        + tiles(2, 2, M, Q, H1)
        + tiles(3, 0, Q, Q, H1)
        + tiles(3, 2, Q, M, H1)
        + tiles(4, 0, M, M, H0)
        + tiles(4, 2, Q, M, H0)
        + tiles(5, 0, Q, Q, H0)
        + tiles(5, 2, M, Q, H0)
    )
    ph3 = (
        tiles(0, 0, M, T, H1)
        + tiles(1, 0, Q, T, H1)
        + tiles(0, 4, T, M, H1)
        + tiles(0, 6, T, Q, H1)
        + tiles(2, 0, T, M, H0)
        + tiles(3, 0, T, Q, H0)
        + tiles(2, 4, M, T, H0)
        + tiles(2, 6, Q, T, H0)
        + tiles(4, 0, T, T, H1)
        + tiles(5, 0, T, T, H0)
    )
    every = ph0 + ph1 + ph2 + ph3
    tab = np.array([(t[2][0], 2 * t[2][1], t[3][0], 2 * t[3][1], t[4]) for t in every], np.int32).T
    xs = (x + s * tab[0] + tab[1] + 8) % SIDE
    ys = (y + s * tab[2] + tab[3] + 8) % SIDE
    where = (xs * SIDE + ys) * TILES + tab[4]
    zs = (z + np.array([2, 2, 0, 0, 0, 0, 0, 0]) + s * np.array([0, 0, 1, -1, -1, 1, 0, 0]) + 8) % SIDE
    blocks = zs * 2 + (core + np.array([0, 1] * 4)) % 2
    idx = jnp.concatenate([where, blocks]).astype(jnp.int32)
    pick = lambda ph: [(t[0], t[1]) for t in ph]

    ft = prep(frontier)
    mine = jnp.concatenate([ft, swap(ft)], 0)
    dx = send(mine, "x")
    dy = send(mine, "y")
    ab = split(adjacency)
    acc = mm(idx, ab, None, [ft], pick(ph0), 0, 4)
    px, py = swap(dx), swap(dy)
    bx = send(dx[:4], "x")
    by = send(dy[:4], "y")
    cx = send(jnp.concatenate([dy[2:4], py[6:8], dy[6:8], py[2:4]], 0), "x")
    cy = send(jnp.concatenate([dx[0:2], px[4:6], dx[4:6], px[0:2]], 0), "y")
    acc = mm(idx, ab, acc, [dx, px, dy, py], pick(ph1), 4, 4)
    pbx, pby = swap(bx[0:2]), swap(by[2:4])
    pcx, pcy = swap(cx[4:8]), swap(cy[4:8])
    ex = send(jnp.concatenate([by[2:4], pby, cx[:4]], 0), "x")
    ey = send(jnp.concatenate([bx[0:2], pbx, cy[:4]], 0), "y")
    acc = mm(idx, ab, acc, [bx, by, cx, pcx, cy, pcy], pick(ph2), 20, 4)
    pex, pey = swap(ex[2:4]), swap(ey[2:4])
    gx, gy = send(ex[:2], "x"), send(ey[:2], "y")
    last = [ex, pex, ey, pey, gx, gy]
    two = mm(idx, ab, acc, last, pick(ph3), 44, 10, 0)
    near = mm(idx, ab, acc, last, pick(ph3), 44, 10, 2)
    back = mm(idx, ab, acc, last, pick(ph3), 44, 10, 4)
    own = mm(idx, ab, acc, last, pick(ph3), 44, 10, 6)
    got2 = send(two[0] + swap(two[1]), "z")
    got1 = send(near[0] + swap(near[1]) + got2, "z")
    got0 = send(back[0] + swap(back[1]), "z", True)
    return finish([own[0], swap(own[1]), got1, got0], visited)


def solution(mesh):
    placed = (P("col", "row"), P(("row", "col"), None), P(None, ("col", "row")))
    return jax.shard_map(
        shards,
        mesh=mesh,
        in_specs=placed,
        out_specs=(P(("col", "row"), None), P(None, ("col", "row"))),
        check_vma=False,
    )
```

```python
import functools

import jax
import jax.numpy as jnp
from jax import lax
from jax.experimental import pallas as pl
from jax.experimental.pallas import tpu as pltpu
from jax.sharding import PartitionSpec as P

SIDE = 4
TILE = 256
CHUNK = 1024
TILES = CHUNK // TILE
BITS = 8

VM = pltpu.VMEM
FULL = pl.BlockSpec(memory_space=VM)

AXES = ("row", "col")


def place(x, y, z, core):
    return (z * 2 + core) * (SIDE * SIDE) + x * SIDE + y


def pairs(axis, flip=False):
    out = []
    for x in range(SIDE):
        for y in range(SIDE):
            for z in range(SIDE):
                for core in range(2):
                    at = [x, y, z]
                    if axis == "core":
                        out.append((place(*at, core), place(*at, 1 - core)))
                        continue
                    n = "xyz".index(axis)
                    step = 1 if (core == 0) != flip else -1
                    to = list(at)
                    to[n] = (to[n] + step) % SIDE
                    out.append((place(*at, core), place(*to, core)))
    return out


def send(value, axis, flip=False):
    return lax.ppermute(value, AXES, pairs(axis, flip))


def swap(value):
    return lax.ppermute(value, AXES, pairs("core"))


def prep_kernel(f_ref, o_ref, s_ref):
    s_ref[...] = f_ref[...].astype(jnp.float32)
    for j in range(TILES):
        rows = []
        for b in range(BITS):
            scale = 2.0**-b if b < 7 else -(2.0**-7)
            rows.append(s_ref[pl.ds(8 * j + b, 32, stride=32), :] * scale)
        o_ref[j] = jnp.concatenate(rows, 0).T.astype(jnp.bfloat16)


def prep(f):
    return pl.pallas_call(
        prep_kernel,
        out_shape=VM((TILES, 128, TILE), jnp.bfloat16),
        in_specs=[FULL],
        out_specs=FULL,
        scratch_shapes=[pltpu.VMEM((CHUNK, 128), jnp.float32)],
        name="prep",
    )(f)


def split_kernel(a_ref, v_ref, o_ref, w_ref):
    r = pl.program_id(0)
    for i in range(a_ref.shape[1] // 128):
        a = a_ref[:, 128 * i : 128 * i + 128]
        for j in range(4):
            part = (lax.shift_right_logical(a, 8 * j) if j else a).astype(jnp.int8).T
            for c in range(4):
                o_ref[r, 16 * i + 4 * c + j] = part[32 * c : 32 * c + 32]
    w_ref[...] = v_ref[...]


def split(adj, visited):
    d, w = adj.shape
    return pl.pallas_call(
        split_kernel,
        grid=(d // 512,),
        in_specs=[pl.BlockSpec((512, w), lambda k: (k, 0)), FULL],
        out_specs=(FULL, FULL),
        out_shape=(VM((d // 512, w // 8, 32, 512), jnp.int8), VM(visited.shape, jnp.int32)),
        compiler_params=pltpu.CompilerParams(vmem_limit_bytes=24 << 20),
        name="split",
    )(pltpu.with_memory_space_constraint(adj, pltpu.HBM), visited)


def here():
    row, col = lax.axis_index("row"), lax.axis_index("col")
    core = row & 1
    return col >> 2, col & 3, row >> 1, core, 1 - 2 * core


def expand(a_ref, r, where):
    parts = []
    for at in where:
        x = a_ref[r, at]
        for b in range(BITS):
            m = 1 << b if b < 7 else -128
            parts.append((x & jnp.int8(m)).astype(jnp.bfloat16))
    return jnp.concatenate(parts, 0)


def mm_kernel(*refs, tiles, arrays, group, blocks, start):
    a_ref, refs = refs[0], refs[1:]
    if not start:
        acc_ref, refs = refs[0], refs[1:]
    f_refs, outs = refs[:arrays], refs[arrays:]
    x, y, z, core, s = here()
    home = {}
    for t in tiles:
        if t[2:4] not in home:
            (a, b), (c, d) = t[2:4]
            home[t[2:4]] = (((x + a * s + 2 * b) & 3) * SIDE + ((y + c * s + 2 * d) & 3)) * TILES
    where = [home[t[2:4]] + t[4] for t in tiles]

    if blocks is not None:
        f = jnp.concatenate([f_refs[t[0]][t[1]] for t in tiles], 1)
        for out, (a, b, other) in zip(outs, blocks):
            r = ((z + a * s + 2 * b) & 3) * 2 + (1 - core if other else core)
            out[...] = acc_ref[r] + jnp.dot(f, expand(a_ref, r, where), preferred_element_type=jnp.float32)
        return

    if len(tiles) == group:
        f = jnp.concatenate([f_refs[t[0]][t[1]] for t in tiles], 1)
        for r in range(8):
            got = jnp.dot(f, expand(a_ref, r, where), preferred_element_type=jnp.float32)
            outs[0][r] = got if start else outs[0][r] + got
        return

    out, scr, at = outs
    for n, t in enumerate(tiles):
        scr[n] = f_refs[t[0]][t[1]]
        at[n] = where[n]

    def step(i, carry):
        base = i * group
        f = jnp.concatenate([scr[base + t] for t in range(group)], 1)
        for r in range(8):
            rhs = expand(a_ref, r, [at[base + t] for t in range(group)])
            out[r] = out[r] + jnp.dot(f, rhs, preferred_element_type=jnp.float32)
        return carry

    lax.fori_loop(0, len(tiles) // group, step, 0)


def mm(ab, acc, arrays, tiles, group, blocks=None):
    count = len(tiles)
    if blocks is None:
        out_shape = VM((8, 128, 512), jnp.float32)
        out_specs = FULL
        lanes = 4096
    else:
        out_shape = (VM((128, 512), jnp.float32),) * len(blocks)
        out_specs = (FULL,) * len(blocks)
        lanes = 512 * len(blocks)
    args = [ab] + ([acc] if acc is not None else []) + list(arrays)
    loop = blocks is None and count != group
    return pl.pallas_call(
        functools.partial(
            mm_kernel, tiles=tuple(tiles), arrays=len(arrays), group=group, blocks=blocks, start=acc is None
        ),
        out_shape=out_shape,
        in_specs=[FULL] * len(args),
        out_specs=out_specs,
        scratch_shapes=[pltpu.VMEM((count, 128, TILE), jnp.bfloat16), pltpu.SMEM((count,), jnp.int32)] if loop else [],
        input_output_aliases={1: 0} if blocks is None and acc is not None else {},
        cost_estimate=pl.CostEstimate(flops=2 * 128 * TILE * count * lanes, bytes_accessed=0, transcendentals=0),
        compiler_params=pltpu.CompilerParams(vmem_limit_bytes=32 << 20),
        name="bits_mm",
    )(*args)


def finish_kernel(a_ref, b_ref, c_ref, d_ref, v_ref, p_ref, o_ref):
    reached = a_ref[...] + b_ref[...] + c_ref[...] + d_ref[...]
    shift = lax.broadcasted_iota(jnp.int32, (32, 1), 0)
    rows = []
    words = []
    for w in range(4):
        got = reached[32 * w : 32 * w + 32]
        word = v_ref[w : w + 1]
        unseen = (lax.shift_right_arithmetic(jnp.broadcast_to(word, got.shape), jnp.broadcast_to(shift, got.shape)) & 1) == 0
        rows.append(jnp.where(unseen, got, 0.0))
        fresh = jnp.where(unseen & (got > 0), lax.shift_left(jnp.int32(1), jnp.broadcast_to(shift, got.shape)), 0)
        words.append(word | jnp.sum(fresh, 0, keepdims=True))
    p_ref[...] = jnp.concatenate(rows, 0).T
    o_ref[...] = jnp.concatenate(words, 0)


def finish(parts, visited):
    return pl.pallas_call(
        finish_kernel,
        out_shape=(jax.ShapeDtypeStruct((512, 128), jnp.float32), jax.ShapeDtypeStruct((4, 512), jnp.int32)),
        in_specs=[FULL] * 5,
        out_specs=(FULL, FULL),
        name="finish",
    )(*parts, visited)


O, M, Q, T = (0, 0), (-1, 0), (1, 0), (0, 1)
H0, H1, ALL = (0, 1), (2, 3), (0, 1, 2, 3)


def tiles(array, start, dx, dy, js):
    return [(array, start + n, dx, dy, j) for n, j in enumerate(js)]


def level(adjacency, frontier, visited):
    ft = prep(frontier)
    mine = jnp.concatenate([ft, swap(ft)], 0)
    dx = send(mine, "x")
    dy = send(mine, "y")
    ab, seen = split(adjacency, visited)
    acc = mm(ab, None, [ft], tiles(0, 0, O, O, ALL), 4)

    bx = send(dx[:4], "x")
    by = send(dy[:4], "y")
    px, py = swap(dx), swap(dy)
    cx = send(jnp.concatenate([dy[2:4], py[6:8], dy[6:8], py[2:4]], 0), "x")
    cy = send(jnp.concatenate([dx[0:2], px[4:6], dx[4:6], px[0:2]], 0), "y")
    near_tiles = (
        tiles(0, 0, M, O, ALL) + tiles(1, 4, Q, O, ALL) + tiles(2, 0, O, M, ALL) + tiles(3, 4, O, Q, ALL)
    )
    acc = mm(ab, acc, [dx, px, dy, py], near_tiles, 8)

    pbx, pby = swap(bx[0:2]), swap(by[2:4])
    ex = send(jnp.concatenate([by[2:4], pby, cx[:4]], 0), "x")
    ey = send(jnp.concatenate([bx[0:2], pbx, cy[:4]], 0), "y")
    pcx, pcy = swap(cx[4:8]), swap(cy[4:8])
    far_tiles = (
        tiles(0, 0, T, O, ALL)
        + tiles(1, 0, O, T, ALL)
        + tiles(2, 0, M, M, H1)
        + tiles(2, 2, M, Q, H1)
        + tiles(3, 0, M, M, H0)
        + tiles(3, 2, Q, M, H0)
    )
    acc = mm(ab, acc, [bx, by, cx, cy], far_tiles, 8)

    gx, gy = send(ex[:2], "x"), send(ey[:2], "y")
    pex, pey = swap(ex[2:4]), swap(ey[2:4])
    side_tiles = tiles(0, 0, Q, Q, H1) + tiles(0, 2, Q, M, H1) + tiles(1, 0, Q, Q, H0) + tiles(1, 2, M, Q, H0)
    acc = mm(ab, acc, [pcx, pcy], side_tiles, 8)

    last = [ex, pex, ey, pey, gx, gy]
    last_tiles = (
        tiles(0, 0, M, T, H1)
        + tiles(1, 0, Q, T, H1)
        + tiles(0, 4, T, M, H1)
        + tiles(0, 6, T, Q, H1)
        + tiles(2, 0, T, M, H0)
        + tiles(3, 0, T, Q, H0)
        + tiles(2, 4, M, T, H0)
        + tiles(2, 6, Q, T, H0)
        + tiles(4, 0, T, T, H1)
        + tiles(5, 0, T, T, H0)
    )
    done = lambda *blocks: mm(ab, acc, last, last_tiles, 20, blocks)
    two, two_o = done((0, 1, False), (0, 1, True))
    up_o, down_o = done((-1, 0, True), (1, 0, True))
    up, down = done((1, 0, False), (-1, 0, False))
    own, own_o = done((0, 0, False), (0, 0, True))
    hop = send(two + swap(two_o), "z")
    got0 = send(down + swap(down_o), "z", True)
    got1 = send(up + swap(up_o) + hop, "z")
    return finish([own, swap(own_o), got1, got0], seen)


def solution(mesh):
    placed = (P("col", "row"), P(("row", "col"), None), P(None, ("col", "row")))
    return jax.shard_map(
        level,
        mesh=mesh,
        in_specs=placed,
        out_specs=(P(("col", "row"), None), P(None, ("col", "row"))),
        check_vma=False,
    )
```

```python
import functools

import jax
import jax.numpy as jnp
from jax import lax
from jax.experimental import pallas as pl
from jax.experimental.pallas import tpu as pltpu
from jax.sharding import PartitionSpec as P


SIDE = 4
TILE = 256
CHUNK = 1024
TILES = CHUNK // TILE
BITS = 8

VM = pltpu.VMEM
FULL = pl.BlockSpec(memory_space=VM)

AXES = ("row", "col")


def place(x, y, z, core):
    return (z * 2 + core) * (SIDE * SIDE) + x * SIDE + y


def pairs(axis, flip=False):
    out = []
    for x in range(SIDE):
        for y in range(SIDE):
            for z in range(SIDE):
                for core in range(2):
                    at = [x, y, z]
                    if axis == "core":
                        out.append((place(*at, core), place(*at, 1 - core)))
                        continue
                    n = "xyz".index(axis)
                    step = 1 if (core == 0) != flip else -1
                    to = list(at)
                    to[n] = (to[n] + step) % SIDE
                    out.append((place(*at, core), place(*to, core)))
    return out


def send(value, axis, flip=False):
    return lax.ppermute(value, AXES, pairs(axis, flip))


def swap(value):
    return lax.ppermute(value, AXES, pairs("core"))


def prep_kernel(f_ref, o_ref, s_ref):
    s_ref[...] = f_ref[...].astype(jnp.float32)
    for j in range(TILES):
        rows = []
        for b in range(BITS):
            scale = 2.0**-b if b < 7 else -(2.0**-7)
            rows.append(s_ref[pl.ds(8 * j + b, 32, stride=32), :] * scale)
        o_ref[j] = jnp.concatenate(rows, 0).T.astype(jnp.bfloat16)


def prep(f):
    return pl.pallas_call(
        prep_kernel,
        out_shape=VM((TILES, 128, TILE), jnp.bfloat16),
        in_specs=[FULL],
        out_specs=FULL,
        scratch_shapes=[pltpu.VMEM((CHUNK, 128), jnp.float32)],
        name="prep",
    )(f)


def split_kernel(a_ref, v_ref, o_ref, w_ref):
    r = pl.program_id(0)
    for i in range(a_ref.shape[1] // 128):
        a = a_ref[:, 128 * i : 128 * i + 128]
        for j in range(4):
            part = (lax.shift_right_logical(a, 8 * j) if j else a).astype(jnp.int8).T
            for c in range(4):
                o_ref[r, 16 * i + 4 * c + j] = part[32 * c : 32 * c + 32]
    w_ref[...] = v_ref[...]


def split(adj, visited):
    d, w = adj.shape
    return pl.pallas_call(
        split_kernel,
        grid=(d // 512,),
        in_specs=[pl.BlockSpec((512, w), lambda k: (k, 0)), FULL],
        out_specs=(FULL, FULL),
        out_shape=(VM((d // 512, w // 8, 32, 512), jnp.int8), VM(visited.shape, jnp.int32)),
        compiler_params=pltpu.CompilerParams(vmem_limit_bytes=24 << 20),
        name="split",
    )(pltpu.with_memory_space_constraint(adj, pltpu.HBM), visited)


def here():
    row, col = lax.axis_index("row"), lax.axis_index("col")
    core = row & 1
    return col >> 2, col & 3, row >> 1, core, 1 - 2 * core


def expand(a_ref, r, where):
    parts = []
    for at in where:
        x = a_ref[r, at]
        for b in range(BITS):
            m = 1 << b if b < 7 else -128
            parts.append((x & jnp.int8(m)).astype(jnp.bfloat16))
    return jnp.concatenate(parts, 0)


def mm_kernel(*refs, tiles, arrays, group, blocks, start):
    n = len(blocks)
    a_ref, refs = refs[0], refs[1:]
    if not start:
        accs, refs = refs[:n], refs[n:]
    f_refs, outs, rest = refs[:arrays], refs[arrays : arrays + n], refs[arrays + n :]
    x, y, z, core, s = here()
    home = {}
    for t in tiles:
        if t[2:4] not in home:
            (a, b), (c, d) = t[2:4]
            home[t[2:4]] = (((x + a * s + 2 * b) & 3) * SIDE + ((y + c * s + 2 * d) & 3)) * TILES
    where = [home[t[2:4]] + t[4] for t in tiles]
    rows = [((z + a * s + 2 * b) & 3) * 2 + (1 - core if other else core) for a, b, other in blocks]

    if len(tiles) == group:
        f = jnp.concatenate([f_refs[t[0]][t[1]] for t in tiles], 1)
        for k in range(n):
            got = jnp.dot(f, expand(a_ref, rows[k], where), preferred_element_type=jnp.float32)
            outs[k][...] = got if start else accs[k][...] + got
        return

    scr, at = rest
    for k, t in enumerate(tiles):
        scr[k] = f_refs[t[0]][t[1]]
        at[k] = where[k]

    def step(i, carry):
        base = i * group
        f = jnp.concatenate([scr[base + t] for t in range(group)], 1)
        for k in range(n):
            rhs = expand(a_ref, rows[k], [at[base + t] for t in range(group)])
            outs[k][...] = outs[k][...] + jnp.dot(f, rhs, preferred_element_type=jnp.float32)
        return carry

    lax.fori_loop(0, len(tiles) // group, step, 0)


def mm(ab, accs, arrays, tiles, group, blocks):
    count, n = len(tiles), len(blocks)
    args = [ab] + list(accs or []) + list(arrays)
    loop = count != group
    return pl.pallas_call(
        functools.partial(
            mm_kernel, tiles=tuple(tiles), arrays=len(arrays), group=group, blocks=tuple(blocks), start=not accs
        ),
        out_shape=(VM((128, 512), jnp.float32),) * n,
        in_specs=[FULL] * len(args),
        out_specs=(FULL,) * n,
        scratch_shapes=[pltpu.VMEM((count, 128, TILE), jnp.bfloat16), pltpu.SMEM((count,), jnp.int32)] if loop else [],
        input_output_aliases={1 + k: k for k in range(n)} if accs else {},
        cost_estimate=pl.CostEstimate(flops=2 * 128 * TILE * count * 512 * n, bytes_accessed=0, transcendentals=0),
        compiler_params=pltpu.CompilerParams(vmem_limit_bytes=32 << 20),
        name="bits_mm",
    )(*args)


def finish_kernel(a_ref, b_ref, c_ref, d_ref, v_ref, p_ref, o_ref):
    reached = a_ref[...] + b_ref[...] + c_ref[...] + d_ref[...]
    shift = lax.broadcasted_iota(jnp.int32, (32, 1), 0)
    rows = []
    words = []
    for w in range(4):
        got = reached[32 * w : 32 * w + 32]
        word = v_ref[w : w + 1]
        unseen = (lax.shift_right_arithmetic(jnp.broadcast_to(word, got.shape), jnp.broadcast_to(shift, got.shape)) & 1) == 0
        rows.append(jnp.where(unseen, got, 0.0))
        fresh = jnp.where(unseen & (got > 0), lax.shift_left(jnp.int32(1), jnp.broadcast_to(shift, got.shape)), 0)
        words.append(word | jnp.sum(fresh, 0, keepdims=True))
    p_ref[...] = jnp.concatenate(rows, 0).T
    o_ref[...] = jnp.concatenate(words, 0)


def finish(parts, visited):
    return pl.pallas_call(
        finish_kernel,
        out_shape=(jax.ShapeDtypeStruct((512, 128), jnp.float32), jax.ShapeDtypeStruct((4, 512), jnp.int32)),
        in_specs=[FULL] * 5,
        out_specs=(FULL, FULL),
        name="finish",
    )(*[pltpu.with_memory_space_constraint(v, VM) for v in (*parts, visited)])


O, M, Q, T = (0, 0), (-1, 0), (1, 0), (0, 1)
H0, H1, ALL = (0, 1), (2, 3), (0, 1, 2, 3)


def tiles(array, start, dx, dy, js):
    return [(array, start + n, dx, dy, j) for n, j in enumerate(js)]


TWO, TWO_O, UP_O, DOWN_O = (0, 1, False), (0, 1, True), (-1, 0, True), (1, 0, True)
UP, DOWN, OWN, OWN_O = (1, 0, False), (-1, 0, False), (0, 0, False), (0, 0, True)
EVERY = (TWO, TWO_O, UP_O, DOWN_O, UP, DOWN, OWN, OWN_O)


def level(adjacency, frontier, visited):
    totals = {}

    def work(arrays, tiles, blocks, group):
        accs = [totals[b] for b in blocks if b in totals]
        got = mm(ab, accs, arrays, tiles, group, blocks)
        totals.update(zip(blocks, got))

    ft = prep(frontier)
    mine = jnp.concatenate([ft, swap(ft)], 0)
    dx = send(mine, "x")
    dy = send(mine, "y")
    ab, seen = split(adjacency, visited)

    px, py = swap(dx), swap(dy)
    bx = send(dx[:4], "x")
    by = send(dy[:4], "y")
    work([ft], tiles(0, 0, O, O, ALL), EVERY, 4)
    cx = send(jnp.concatenate([dy[2:4], py[6:8], dy[6:8], py[2:4]], 0), "x")
    cy = send(jnp.concatenate([dx[0:2], px[4:6], dx[4:6], px[0:2]], 0), "y")
    work([dx, dy], tiles(0, 0, M, O, ALL) + tiles(1, 0, O, M, ALL), EVERY, 8)

    pbx, pby = swap(bx[0:2]), swap(by[2:4])
    work([px, py], tiles(0, 4, Q, O, ALL) + tiles(1, 4, O, Q, ALL), EVERY, 8)
    ex = send(jnp.concatenate([by[2:4], pby], 0), "x")
    ey = send(jnp.concatenate([bx[0:2], pbx], 0), "y")
    hx, hy = send(cx[:4], "x"), send(cy[:4], "y")
    pcx, pcy = swap(cx[4:8]), swap(cy[4:8])
    work([bx, by], tiles(0, 0, T, O, ALL) + tiles(1, 0, O, T, ALL), EVERY, 8)

    gx, gy = send(ex[:2], "x"), send(ey[:2], "y")
    pex, pey = swap(ex[2:4]), swap(ey[2:4])

    late = [cx, cy, pcx, pcy, ex, ey, pex, pey, hx, hy, gx, gy]
    fb = tiles(0, 0, M, M, H1) + tiles(0, 2, M, Q, H1) + tiles(1, 0, M, M, H0) + tiles(1, 2, Q, M, H0)
    sd = tiles(2, 0, Q, Q, H1) + tiles(2, 2, Q, M, H1) + tiles(3, 0, Q, Q, H0) + tiles(3, 2, M, Q, H0)
    sd = sd + tiles(4, 0, M, T, H1) + tiles(5, 0, T, M, H0) + tiles(6, 0, Q, T, H1) + tiles(7, 0, T, Q, H0)
    la = tiles(8, 0, T, M, H1) + tiles(8, 2, T, Q, H1) + tiles(9, 0, M, T, H0) + tiles(9, 2, Q, T, H0)
    la = la + tiles(10, 0, T, T, H1) + tiles(11, 0, T, T, H0)

    def late_work(tiles, blocks, group):
        used = sorted({t[0] for t in tiles})
        work([late[n] for n in used], [(used.index(t[0]),) + t[1:] for t in tiles], blocks, group)

    first = EVERY[:4]
    late_work(fb, first, 8)
    late_work(sd, first, 8)
    late_work(la, (TWO, TWO_O), 12)
    late_work(la, (UP_O, DOWN_O), 12)
    late_work(fb + sd + la, (UP, DOWN), 36)
    late_work(fb + sd + la, (OWN, OWN_O), 36)

    hop = send(totals[TWO] + swap(totals[TWO_O]), "z")
    got0 = send(totals[DOWN] + swap(totals[DOWN_O]), "z", True)
    got1 = send(totals[UP] + swap(totals[UP_O]) + hop, "z")
    rest = swap(totals[OWN_O])
    return finish([totals[OWN], rest, got1, got0], seen)


def solution(mesh):
    placed = (P("col", "row"), P(("row", "col"), None), P(None, ("col", "row")))
    return jax.shard_map(
        level,
        mesh=mesh,
        in_specs=placed,
        out_specs=(P(("col", "row"), None), P(None, ("col", "row"))),
        check_vma=False,
    )
```

```python
import functools

import jax
import jax.numpy as jnp
from jax import lax
from jax.experimental import pallas as pl
from jax.experimental.pallas import tpu as pltpu
from jax.sharding import PartitionSpec as P


SIDE = 4
TILE = 256
CHUNK = 1024
TILES = CHUNK // TILE
BITS = 8

VM = pltpu.VMEM
FULL = pl.BlockSpec(memory_space=VM)

AXES = ("row", "col")


def place(x, y, z, core):
    return (z * 2 + core) * (SIDE * SIDE) + x * SIDE + y


def pairs(axis, flip=False):
    out = []
    for x in range(SIDE):
        for y in range(SIDE):
            for z in range(SIDE):
                for core in range(2):
                    at = [x, y, z]
                    if axis == "core":
                        out.append((place(*at, core), place(*at, 1 - core)))
                        continue
                    n = "xyz".index(axis)
                    step = 1 if (core == 0) != flip else -1
                    to = list(at)
                    to[n] = (to[n] + step) % SIDE
                    out.append((place(*at, core), place(*to, core)))
    return out


def send(value, axis, flip=False):
    return lax.ppermute(value, AXES, pairs(axis, flip))


def swap(value):
    return lax.ppermute(value, AXES, pairs("core"))


def prep_kernel(f_ref, o_ref, s_ref):
    s_ref[...] = f_ref[...].astype(jnp.float32)
    for j in range(TILES):
        rows = []
        for b in range(BITS):
            scale = 2.0**-b if b < 7 else -(2.0**-7)
            rows.append(s_ref[pl.ds(8 * j + b, 32, stride=32), :] * scale)
        o_ref[j] = jnp.concatenate(rows, 0).T.astype(jnp.bfloat16)


def prep(f):
    return pl.pallas_call(
        prep_kernel,
        out_shape=VM((TILES, 128, TILE), jnp.bfloat16),
        in_specs=[FULL],
        out_specs=FULL,
        scratch_shapes=[pltpu.VMEM((CHUNK, 128), jnp.float32)],
        name="prep",
    )(f)


def split_kernel(a_ref, v_ref, o_ref, w_ref):
    r = pl.program_id(0)
    for i in range(a_ref.shape[1] // 128):
        a = a_ref[:, 128 * i : 128 * i + 128]
        for j in range(4):
            part = (lax.shift_right_logical(a, 8 * j) if j else a).astype(jnp.int8).T
            for c in range(4):
                o_ref[r, 16 * i + 4 * c + j] = part[32 * c : 32 * c + 32]
    w_ref[...] = v_ref[...]


def split(adj, visited):
    d, w = adj.shape
    return pl.pallas_call(
        split_kernel,
        grid=(d // 512,),
        in_specs=[pl.BlockSpec((512, w), lambda k: (k, 0)), pl.BlockSpec(visited.shape, lambda k: (0, 0))],
        out_specs=(FULL, FULL),
        out_shape=(VM((d // 512, w // 8, 32, 512), jnp.int8), VM(visited.shape, jnp.int32)),
        compiler_params=pltpu.CompilerParams(vmem_limit_bytes=24 << 20),
        name="split",
    )(*[pltpu.with_memory_space_constraint(v, pltpu.HBM) for v in (adj, visited)])


def here():
    row, col = lax.axis_index("row"), lax.axis_index("col")
    core = row & 1
    return col >> 2, col & 3, row >> 1, core, 1 - 2 * core


def expand(a_ref, r, where):
    parts = []
    for at in where:
        x = a_ref[r, at]
        for b in range(BITS):
            m = 1 << b if b < 7 else -128
            parts.append((x & jnp.int8(m)).astype(jnp.bfloat16))
    return jnp.concatenate(parts, 0)


def mm_kernel(*refs, tiles, arrays, group, blocks, start):
    n = len(blocks)
    a_ref, refs = refs[0], refs[1:]
    if not start:
        accs, refs = refs[:n], refs[n:]
    f_refs, outs, rest = refs[:arrays], refs[arrays : arrays + n], refs[arrays + n :]
    x, y, z, core, s = here()
    home = {}
    for t in tiles:
        if t[2:4] not in home:
            (a, b), (c, d) = t[2:4]
            home[t[2:4]] = (((x + a * s + 2 * b) & 3) * SIDE + ((y + c * s + 2 * d) & 3)) * TILES
    where = [home[t[2:4]] + t[4] for t in tiles]
    rows = [((z + a * s + 2 * b) & 3) * 2 + (1 - core if other else core) for a, b, other in blocks]

    if len(tiles) == group:
        f = jnp.concatenate([f_refs[t[0]][t[1]] for t in tiles], 1)
        for k in range(n):
            got = jnp.dot(f, expand(a_ref, rows[k], where), preferred_element_type=jnp.float32)
            outs[k][...] = got if start else accs[k][...] + got
        return

    scr, at = rest
    for k, t in enumerate(tiles):
        scr[k] = f_refs[t[0]][t[1]]
        at[k] = where[k]

    if start:
        for k in range(n):
            outs[k][...] = jnp.zeros_like(outs[k])

    def step(i, carry):
        base = i * group
        f = jnp.concatenate([scr[base + t] for t in range(group)], 1)
        for k in range(n):
            rhs = expand(a_ref, rows[k], [at[base + t] for t in range(group)])
            outs[k][...] = outs[k][...] + jnp.dot(f, rhs, preferred_element_type=jnp.float32)
        return carry

    lax.fori_loop(0, len(tiles) // group, step, 0)


def mm(ab, accs, arrays, tiles, group, blocks):
    count, n = len(tiles), len(blocks)
    args = [ab] + list(accs or []) + list(arrays)
    loop = count != group
    return pl.pallas_call(
        functools.partial(
            mm_kernel, tiles=tuple(tiles), arrays=len(arrays), group=group, blocks=tuple(blocks), start=not accs
        ),
        out_shape=(VM((128, 512), jnp.float32),) * n,
        in_specs=[FULL] * len(args),
        out_specs=(FULL,) * n,
        scratch_shapes=[pltpu.VMEM((count, 128, TILE), jnp.bfloat16), pltpu.SMEM((count,), jnp.int32)] if loop else [],
        input_output_aliases={1 + k: k for k in range(n)} if accs else {},
        cost_estimate=pl.CostEstimate(flops=2 * 128 * TILE * count * 512 * n, bytes_accessed=0, transcendentals=0),
        compiler_params=pltpu.CompilerParams(vmem_limit_bytes=32 << 20),
        name="bits_mm",
    )(*args)


def finish_kernel(a_ref, b_ref, c_ref, d_ref, v_ref, p_ref, o_ref):
    reached = a_ref[...] + b_ref[...] + c_ref[...] + d_ref[...]
    shift = lax.broadcasted_iota(jnp.int32, (32, 1), 0)
    rows = []
    words = []
    for w in range(4):
        got = reached[32 * w : 32 * w + 32]
        word = v_ref[w : w + 1]
        unseen = (lax.shift_right_arithmetic(jnp.broadcast_to(word, got.shape), jnp.broadcast_to(shift, got.shape)) & 1) == 0
        rows.append(jnp.where(unseen, got, 0.0))
        fresh = jnp.where(unseen & (got > 0), lax.shift_left(jnp.int32(1), jnp.broadcast_to(shift, got.shape)), 0)
        words.append(word | jnp.sum(fresh, 0, keepdims=True))
    p_ref[...] = jnp.concatenate(rows, 0).T
    o_ref[...] = jnp.concatenate(words, 0)


def finish(parts, visited):
    return pl.pallas_call(
        finish_kernel,
        out_shape=(jax.ShapeDtypeStruct((512, 128), jnp.float32), jax.ShapeDtypeStruct((4, 512), jnp.int32)),
        in_specs=[FULL] * 5,
        out_specs=(FULL, FULL),
        name="finish",
    )(*[pltpu.with_memory_space_constraint(v, VM) for v in (*parts, visited)])


O, M, Q, T = (0, 0), (-1, 0), (1, 0), (0, 1)
H0, H1, ALL = (0, 1), (2, 3), (0, 1, 2, 3)


def tiles(array, start, dx, dy, js):
    return [(array, start + n, dx, dy, j) for n, j in enumerate(js)]


TWO, TWO_O, UP_O, DOWN_O = (0, 1, False), (0, 1, True), (-1, 0, True), (1, 0, True)
UP, DOWN, OWN, OWN_O = (1, 0, False), (-1, 0, False), (0, 0, False), (0, 0, True)
SOON = (TWO, TWO_O, DOWN_O, UP_O, DOWN)


def level(adjacency, frontier, visited):
    totals = {}

    def work(arrays, tiles, blocks, group):
        accs = [totals[b] for b in blocks if b in totals]
        got = mm(ab, accs, arrays, tiles, group, blocks)
        totals.update(zip(blocks, got))

    ft = prep(frontier)
    mine = jnp.concatenate([ft, swap(ft)], 0)
    dx = send(mine, "x")
    dy = send(mine, "y")
    ab, seen = split(adjacency, visited)

    px, py = swap(dx), swap(dy)
    bx = send(dx[:4], "x")
    by = send(dy[:4], "y")
    work([ft], tiles(0, 0, O, O, ALL), SOON, 4)
    cx = send(jnp.concatenate([dy[2:4], py[6:8], dy[6:8], py[2:4]], 0), "x")
    cy = send(jnp.concatenate([dx[0:2], px[4:6], dx[4:6], px[0:2]], 0), "y")
    work([dx], tiles(0, 0, M, O, ALL), SOON, 4)

    pb = swap(jnp.concatenate([bx[0:2], by[2:4]], 0))
    work([dy], tiles(0, 0, O, M, ALL), SOON, 4)
    ex = send(jnp.concatenate([by[2:4], pb[2:4]], 0), "x")
    ey = send(jnp.concatenate([bx[0:2], pb[0:2]], 0), "y")
    work([px, py], tiles(0, 4, Q, O, ALL) + tiles(1, 4, O, Q, ALL), SOON, 8)

    pc = swap(jnp.concatenate([cx[4:8], cy[4:8]], 0))
    hx, hy = send(cx[:4], "x"), send(cy[:4], "y")
    gx, gy = send(ex[:2], "x"), send(ey[:2], "y")
    pe = swap(jnp.concatenate([ex[2:4], ey[2:4]], 0))
    work([bx, by], tiles(0, 0, T, O, ALL) + tiles(1, 0, O, T, ALL), SOON, 8)

    arrays = [ft, dx, px, dy, py, bx, by, cx, cy, pc, ex, ey, pe, hx, hy, gx, gy]
    ea = tiles(0, 0, O, O, ALL) + tiles(1, 0, M, O, ALL) + tiles(2, 4, Q, O, ALL) + tiles(3, 0, O, M, ALL)
    ea = ea + tiles(4, 4, O, Q, ALL) + tiles(5, 0, T, O, ALL) + tiles(6, 0, O, T, ALL)
    fb = tiles(7, 0, M, M, H1) + tiles(7, 2, M, Q, H1) + tiles(8, 0, M, M, H0) + tiles(8, 2, Q, M, H0)
    sd = tiles(9, 0, Q, Q, H1) + tiles(9, 2, Q, M, H1) + tiles(9, 4, Q, Q, H0) + tiles(9, 6, M, Q, H0)
    sd = sd + tiles(10, 0, M, T, H1) + tiles(11, 0, T, M, H0) + tiles(12, 0, Q, T, H1) + tiles(12, 2, T, Q, H0)
    la = tiles(13, 0, T, M, H1) + tiles(13, 2, T, Q, H1) + tiles(14, 0, M, T, H0) + tiles(14, 2, Q, T, H0)
    la = la + tiles(15, 0, T, T, H1) + tiles(16, 0, T, T, H0)

    def late_work(tiles, blocks, group):
        used = sorted({t[0] for t in tiles})
        work([arrays[n] for n in used], [(used.index(t[0]),) + t[1:] for t in tiles], blocks, group)

    late_work(fb, SOON, 8)
    late_work(sd, (TWO, TWO_O), 16)
    late_work(la, (TWO, TWO_O), 12)
    late_work(sd + la, (DOWN_O,), 28)
    late_work(sd + la, (DOWN,), 28)
    late_work(sd + la, (UP_O,), 28)
    late_work(ea + fb + sd + la, (UP,), 64)
    late_work(ea + fb + sd + la, (OWN_O,), 64)
    late_work(ea + fb + sd + la, (OWN,), 64)

    hop = send(totals[TWO] + swap(totals[TWO_O]), "z")
    got0 = send(totals[DOWN] + swap(totals[DOWN_O]), "z", True)
    got1 = send(totals[UP] + swap(totals[UP_O]) + hop, "z")
    rest = swap(totals[OWN_O])
    return finish([totals[OWN], rest, got1, got0], seen)


def solution(mesh):
    placed = (P("col", "row"), P(("row", "col"), None), P(None, ("col", "row")))
    return jax.shard_map(
        level,
        mesh=mesh,
        in_specs=placed,
        out_specs=(P(("col", "row"), None), P(None, ("col", "row"))),
        check_vma=False,
    )
```

```python
import functools

import jax
import jax.numpy as jnp
from jax import lax
from jax.experimental import pallas as pl
from jax.experimental.pallas import tpu as pltpu
from jax.sharding import PartitionSpec as P


SIDE = 4
TILE = 256
CHUNK = 1024
TILES = CHUNK // TILE
BITS = 8

VM = pltpu.VMEM
FULL = pl.BlockSpec(memory_space=VM)

AXES = ("row", "col")


def place(x, y, z, core):
    return (z * 2 + core) * (SIDE * SIDE) + x * SIDE + y


def pairs(axis, flip=False):
    out = []
    for x in range(SIDE):
        for y in range(SIDE):
            for z in range(SIDE):
                for core in range(2):
                    at = [x, y, z]
                    if axis == "core":
                        out.append((place(*at, core), place(*at, 1 - core)))
                        continue
                    n = "xyz".index(axis)
                    step = 1 if (core == 0) != flip else -1
                    to = list(at)
                    to[n] = (to[n] + step) % SIDE
                    out.append((place(*at, core), place(*to, core)))
    return out


def send(value, axis, flip=False):
    return lax.ppermute(value, AXES, pairs(axis, flip))


def swap(value):
    return lax.ppermute(value, AXES, pairs("core"))


def prep_kernel(f_ref, o_ref, s_ref):
    s_ref[...] = f_ref[...].astype(jnp.float32)
    for j in range(TILES):
        rows = []
        for b in range(BITS):
            scale = 2.0**-b if b < 7 else -(2.0**-7)
            rows.append(s_ref[pl.ds(8 * j + b, 32, stride=32), :] * scale)
        o_ref[j] = jnp.concatenate(rows, 0).T.astype(jnp.bfloat16)


def prep(f):
    return pl.pallas_call(
        prep_kernel,
        out_shape=VM((TILES, 128, TILE), jnp.bfloat16),
        in_specs=[FULL],
        out_specs=FULL,
        scratch_shapes=[pltpu.VMEM((CHUNK, 128), jnp.float32)],
        name="prep",
    )(f)


def split_kernel(a_hbm, v_hbm, o_ref, w_ref, buf, sem):
    rows = a_hbm.shape[0] // 512

    def fetch(r):
        return pltpu.make_async_copy(a_hbm.at[pl.ds(pl.multiple_of(512 * r, 512), 512)], buf.at[r], sem.at[r])

    for r in range(rows):
        fetch(r).start()
    seen = pltpu.make_async_copy(v_hbm, w_ref, sem.at[rows])
    seen.start()

    def step(r, carry):
        fetch(r).wait()
        for i in range(buf.shape[2] // 128):
            a = buf[r, :, 128 * i : 128 * i + 128]
            for j in range(4):
                part = (lax.shift_right_logical(a, 8 * j) if j else a).astype(jnp.int8).T
                for c in range(4):
                    o_ref[r, 16 * i + 4 * c + j] = part[32 * c : 32 * c + 32]
        return carry

    lax.fori_loop(0, rows, step, 0)
    seen.wait()


def split(adj, visited):
    d, w = adj.shape
    return pl.pallas_call(
        split_kernel,
        in_specs=[pl.BlockSpec(memory_space=pltpu.HBM)] * 2,
        out_specs=(FULL, FULL),
        out_shape=(VM((d // 512, w // 8, 32, 512), jnp.int8), VM(visited.shape, jnp.int32)),
        scratch_shapes=[pltpu.VMEM((d // 512, 512, w), jnp.int32), pltpu.SemaphoreType.DMA((d // 512 + 1,))],
        compiler_params=pltpu.CompilerParams(vmem_limit_bytes=32 << 20),
        name="split",
    )(*[pltpu.with_memory_space_constraint(v, pltpu.HBM) for v in (adj, visited)])


def here():
    row, col = lax.axis_index("row"), lax.axis_index("col")
    core = row & 1
    return col >> 2, col & 3, row >> 1, core, 1 - 2 * core


def expand(a_ref, r, where):
    parts = []
    for at in where:
        x = a_ref[r, at]
        for b in range(BITS):
            m = 1 << b if b < 7 else -128
            parts.append((x & jnp.int8(m)).astype(jnp.bfloat16))
    return jnp.concatenate(parts, 0)


def mm_kernel(*refs, jobs, arrays, started):
    a_ref, refs = refs[0], refs[1:]
    count = sum(started)
    accs, f_refs, outs = iter(refs[:count]), refs[count : count + arrays], refs[count + arrays :]
    x, y, z, core, s = here()
    where, left = {}, {}
    for _, tiles in jobs:
        for t in tiles:
            if t[2:4] not in where:
                (a, b), (c, d) = t[2:4]
                where[t[2:4]] = (((x + a * s + 2 * b) & 3) * SIDE + ((y + c * s + 2 * d) & 3)) * TILES
    for ((a, b, other), tiles), out, has in zip(jobs, outs, started):
        r = ((z + a * s + 2 * b) & 3) * 2 + (1 - core if other else core)
        if tiles not in left:
            left[tiles] = jnp.concatenate([f_refs[t[0]][t[1]] for t in tiles], 1)
        right = expand(a_ref, r, [where[t[2:4]] + t[4] for t in tiles])
        got = jnp.dot(left[tiles], right, preferred_element_type=jnp.float32)
        out[...] = next(accs)[...] + got if has else got


def mm(ab, accs, arrays, jobs):
    started = tuple(a is not None for a in accs)
    olds = [a for a in accs if a is not None]
    count = sum(len(t) for _, t in jobs)
    alias, k = {}, 0
    for n, has in enumerate(started):
        if has:
            k += 1
            alias[k] = n
    args = [ab] + olds + list(arrays)
    return pl.pallas_call(
        functools.partial(mm_kernel, jobs=jobs, arrays=len(arrays), started=started),
        out_shape=(VM((128, 512), jnp.float32),) * len(jobs),
        in_specs=[FULL] * len(args),
        out_specs=(FULL,) * len(jobs),
        input_output_aliases=alias,
        cost_estimate=pl.CostEstimate(flops=2 * 128 * TILE * count * 512, bytes_accessed=0, transcendentals=0),
        compiler_params=pltpu.CompilerParams(vmem_limit_bytes=32 << 20),
        name="bits_mm",
    )(*args)


def finish_kernel(a_ref, b_ref, c_ref, d_ref, v_ref, p_ref, o_ref):
    reached = a_ref[...] + b_ref[...] + c_ref[...] + d_ref[...]
    shift = lax.broadcasted_iota(jnp.int32, (32, 1), 0)
    rows = []
    words = []
    for w in range(4):
        got = reached[32 * w : 32 * w + 32]
        word = v_ref[w : w + 1]
        unseen = (lax.shift_right_arithmetic(jnp.broadcast_to(word, got.shape), jnp.broadcast_to(shift, got.shape)) & 1) == 0
        rows.append(jnp.where(unseen, got, 0.0))
        fresh = jnp.where(unseen & (got > 0), lax.shift_left(jnp.int32(1), jnp.broadcast_to(shift, got.shape)), 0)
        words.append(word | jnp.sum(fresh, 0, keepdims=True))
    p_ref[...] = jnp.concatenate(rows, 0).T
    o_ref[...] = jnp.concatenate(words, 0)


def finish(parts, visited):
    return pl.pallas_call(
        finish_kernel,
        out_shape=(jax.ShapeDtypeStruct((512, 128), jnp.float32), jax.ShapeDtypeStruct((4, 512), jnp.int32)),
        in_specs=[FULL] * 5,
        out_specs=(FULL, FULL),
        name="finish",
    )(*[pltpu.with_memory_space_constraint(v, VM) for v in (*parts, visited)])


O, M, Q, T = (0, 0), (-1, 0), (1, 0), (0, 1)
H0, H1, ALL = (0, 1), (2, 3), (0, 1, 2, 3)


def tiles(array, start, dx, dy, js):
    return tuple((array, start + n, dx, dy, j) for n, j in enumerate(js))


TWO, TWO_O, UP_O, DOWN_O = (0, 1, False), (0, 1, True), (-1, 0, True), (1, 0, True)
UP, DOWN, OWN, OWN_O = (1, 0, False), (-1, 0, False), (0, 0, False), (0, 0, True)
SOON = (TWO, TWO_O, DOWN_O, UP_O, DOWN)


def level(adjacency, frontier, visited):
    totals = {}

    def work(*jobs):
        used = sorted({t[0] for ts, _ in jobs for t in ts})
        each = tuple(
            (b, tuple((used.index(t[0]),) + t[1:] for t in ts)) for ts, blocks in jobs for b in blocks
        )
        got = mm(ab, [totals.get(b) for b, _ in each], [arrays[n] for n in used], each)
        totals.update(zip([b for b, _ in each], got))

    ft = prep(frontier)
    theirs = swap(ft)
    dx, dy = send(ft, "x"), send(ft, "y")
    ox, oy = send(theirs, "x"), send(theirs, "y")
    ab, seen = split(adjacency, visited)

    bx, by = send(dx, "x"), send(dy, "y")
    po = swap(jnp.concatenate([dx[0:2], dy[2:4]], 0))
    pn = swap(jnp.concatenate([ox, oy], 0))
    cx = send(jnp.concatenate([dy[2:4], pn[6:8], oy[2:4], po[2:4]], 0), "x")
    cy = send(jnp.concatenate([dx[0:2], pn[0:2], ox[0:2], po[0:2]], 0), "y")
    pb = swap(jnp.concatenate([bx[0:2], by[2:4]], 0))
    ex = send(jnp.concatenate([by[2:4], pb[2:4]], 0), "x")
    ey = send(jnp.concatenate([bx[0:2], pb[0:2]], 0), "y")
    hx, hy = send(cx[:4], "x"), send(cy[:4], "y")
    pc = swap(jnp.concatenate([cx[4:8], cy[4:8]], 0))
    gx, gy = send(ex[:2], "x"), send(ey[:2], "y")
    pe = swap(jnp.concatenate([ex[2:4], ey[2:4]], 0))
    arrays = [ft, dx, pn, dy, bx, by, cx, cy, pc, ex, ey, pe, hx, hy, gx, gy]

    own = tiles(0, 0, O, O, ALL)
    n1, n2 = tiles(1, 0, M, O, ALL), tiles(3, 0, O, M, ALL)
    n3, n4 = tiles(2, 0, Q, O, ALL), tiles(2, 4, O, Q, ALL)
    fa = tiles(4, 0, T, O, ALL) + tiles(5, 0, O, T, ALL)
    fb = tiles(6, 0, M, M, H1) + tiles(6, 2, M, Q, H1) + tiles(7, 0, M, M, H0) + tiles(7, 2, Q, M, H0)
    sd = tiles(8, 0, Q, Q, H1) + tiles(8, 2, Q, M, H1) + tiles(8, 4, Q, Q, H0) + tiles(8, 6, M, Q, H0)
    sd = sd + tiles(9, 0, M, T, H1) + tiles(10, 0, T, M, H0) + tiles(11, 0, Q, T, H1) + tiles(11, 2, T, Q, H0)
    la = tiles(12, 0, T, M, H1) + tiles(12, 2, T, Q, H1) + tiles(13, 0, M, T, H0) + tiles(13, 2, Q, T, H0)
    la = la + tiles(14, 0, T, T, H1) + tiles(15, 0, T, T, H0)
    rest = n1 + n2 + n3 + n4 + fa + fb + sd + la

    work((own, SOON))
    work((n1, SOON))
    work((n2, SOON))
    work((n3, SOON))
    work((n4, SOON))
    work((fa, SOON))
    work((fb, SOON))
    work((sd, (TWO, TWO_O)))
    work((la, (TWO_O, TWO)))
    work((sd + la, (DOWN_O,)))
    work((sd + la, (DOWN,)))
    work((sd + la, (UP_O,)))
    work((own + rest, (UP,)))
    work((own + rest, (OWN_O,)))
    work((own + rest, (OWN,)))

    hop = send(totals[TWO] + swap(totals[TWO_O]), "z")
    got0 = send(totals[DOWN] + swap(totals[DOWN_O]), "z", True)
    got1 = send(totals[UP] + swap(totals[UP_O]) + hop, "z")
    last = swap(totals[OWN_O])
    return finish([totals[OWN], last, got1, got0], seen)


def solution(mesh):
    placed = (P("col", "row"), P(("row", "col"), None), P(None, ("col", "row")))
    return jax.shard_map(
        level,
        mesh=mesh,
        in_specs=placed,
        out_specs=(P(("col", "row"), None), P(None, ("col", "row"))),
        check_vma=False,
    )
```

```python
import functools

import jax
import jax.numpy as jnp
from jax import lax
from jax.experimental import pallas as pl
from jax.experimental.pallas import tpu as pltpu
from jax.sharding import PartitionSpec as P


SIDE = 4
TILE = 256
CHUNK = 1024
TILES = CHUNK // TILE
BITS = 8

VM = pltpu.VMEM
FULL = pl.BlockSpec(memory_space=VM)

AXES = ("row", "col")


def place(x, y, z, core):
    return (z * 2 + core) * (SIDE * SIDE) + x * SIDE + y


def pairs(axis, flip=False):
    out = []
    for x in range(SIDE):
        for y in range(SIDE):
            for z in range(SIDE):
                for core in range(2):
                    at = [x, y, z]
                    if axis == "core":
                        out.append((place(*at, core), place(*at, 1 - core)))
                        continue
                    n = "xyz".index(axis)
                    step = 1 if (core == 0) != flip else -1
                    to = list(at)
                    to[n] = (to[n] + step) % SIDE
                    out.append((place(*at, core), place(*to, core)))
    return out


def send(value, axis, flip=False):
    return lax.ppermute(value, AXES, pairs(axis, flip))


def swap(value):
    return lax.ppermute(value, AXES, pairs("core"))


def prep_kernel(f_ref, o_ref, s_ref):
    s_ref[...] = f_ref[...].astype(jnp.float32)
    for j in range(TILES):
        rows = []
        for b in range(BITS):
            scale = 2.0**-b if b < 7 else -(2.0**-7)
            rows.append(s_ref[pl.ds(8 * j + b, 32, stride=32), :] * scale)
        o_ref[j] = jnp.concatenate(rows, 0).T.astype(jnp.bfloat16)


def prep(f):
    return pl.pallas_call(
        prep_kernel,
        out_shape=VM((TILES, 128, TILE), jnp.bfloat16),
        in_specs=[FULL],
        out_specs=FULL,
        scratch_shapes=[pltpu.VMEM((CHUNK, 128), jnp.float32)],
        name="prep",
    )(f)


def split_kernel(a_hbm, v_hbm, o_ref, w_ref, buf, sem):
    rows = a_hbm.shape[0] // 512

    def fetch(r):
        return pltpu.make_async_copy(a_hbm.at[pl.ds(pl.multiple_of(512 * r, 512), 512)], buf.at[r], sem.at[r])

    for r in range(rows):
        fetch(r).start()
    seen = pltpu.make_async_copy(v_hbm, w_ref, sem.at[rows])
    seen.start()

    def step(r, carry):
        fetch(r).wait()
        for i in range(buf.shape[2] // 128):
            a = buf[r, :, 128 * i : 128 * i + 128]
            for j in range(4):
                part = (lax.shift_right_logical(a, 8 * j) if j else a).astype(jnp.int8).T
                for c in range(4):
                    o_ref[r, 16 * i + 4 * c + j] = part[32 * c : 32 * c + 32]
        return carry

    lax.fori_loop(0, rows, step, 0)
    seen.wait()


def split(adj, visited):
    d, w = adj.shape
    return pl.pallas_call(
        split_kernel,
        in_specs=[pl.BlockSpec(memory_space=pltpu.HBM)] * 2,
        out_specs=(FULL, FULL),
        out_shape=(VM((d // 512, w // 8, 32, 512), jnp.int8), VM(visited.shape, jnp.int32)),
        scratch_shapes=[pltpu.VMEM((d // 512, 512, w), jnp.int32), pltpu.SemaphoreType.DMA((d // 512 + 1,))],
        compiler_params=pltpu.CompilerParams(vmem_limit_bytes=32 << 20),
        name="split",
    )(*[pltpu.with_memory_space_constraint(v, pltpu.HBM) for v in (adj, visited)])


def here():
    row, col = lax.axis_index("row"), lax.axis_index("col")
    core = row & 1
    return col >> 2, col & 3, row >> 1, core, 1 - 2 * core


def expand(a_ref, r, where):
    parts = []
    for at in where:
        x = a_ref[r, at]
        for b in range(BITS):
            m = 1 << b if b < 7 else -128
            parts.append((x & jnp.int8(m)).astype(jnp.bfloat16))
    return jnp.concatenate(parts, 0)


def mm_kernel(*refs, jobs, arrays, started):
    a_ref, refs = refs[0], refs[1:]
    count = sum(started)
    accs, f_refs, outs = iter(refs[:count]), refs[count : count + arrays], refs[count + arrays :]
    x, y, z, core, s = here()
    where, left = {}, {}
    for _, tiles in jobs:
        for t in tiles:
            if t[2:4] not in where:
                (a, b), (c, d) = t[2:4]
                where[t[2:4]] = (((x + a * s + 2 * b) & 3) * SIDE + ((y + c * s + 2 * d) & 3)) * TILES
    for ((a, b, other), tiles), out, has in zip(jobs, outs, started):
        r = ((z + a * s + 2 * b) & 3) * 2 + (1 - core if other else core)
        if tiles not in left:
            left[tiles] = jnp.concatenate([f_refs[t[0]][t[1]] for t in tiles], 1)
        right = expand(a_ref, r, [where[t[2:4]] + t[4] for t in tiles])
        got = jnp.dot(left[tiles], right, preferred_element_type=jnp.float32)
        out[...] = next(accs)[...] + got if has else got


def mm(ab, accs, arrays, jobs):
    started = tuple(a is not None for a in accs)
    olds = [a for a in accs if a is not None]
    count = sum(len(t) for _, t in jobs)
    alias, k = {}, 0
    for n, has in enumerate(started):
        if has:
            k += 1
            alias[k] = n
    args = [ab] + olds + list(arrays)
    return pl.pallas_call(
        functools.partial(mm_kernel, jobs=jobs, arrays=len(arrays), started=started),
        out_shape=(VM((128, 512), jnp.float32),) * len(jobs),
        in_specs=[FULL] * len(args),
        out_specs=(FULL,) * len(jobs),
        input_output_aliases=alias,
        cost_estimate=pl.CostEstimate(flops=2 * 128 * TILE * count * 512, bytes_accessed=0, transcendentals=0),
        compiler_params=pltpu.CompilerParams(vmem_limit_bytes=32 << 20),
        name="bits_mm",
    )(*args)


def finish_kernel(a_ref, b_ref, c_ref, d_ref, v_ref, p_ref, o_ref):
    reached = a_ref[...] + b_ref[...] + c_ref[...] + d_ref[...]
    shift = lax.broadcasted_iota(jnp.int32, (32, 1), 0)
    rows = []
    words = []
    for w in range(4):
        got = reached[32 * w : 32 * w + 32]
        word = v_ref[w : w + 1]
        unseen = (lax.shift_right_arithmetic(jnp.broadcast_to(word, got.shape), jnp.broadcast_to(shift, got.shape)) & 1) == 0
        rows.append(jnp.where(unseen, got, 0.0))
        fresh = jnp.where(unseen & (got > 0), lax.shift_left(jnp.int32(1), jnp.broadcast_to(shift, got.shape)), 0)
        words.append(word | jnp.sum(fresh, 0, keepdims=True))
    p_ref[...] = jnp.concatenate(rows, 0).T
    o_ref[...] = jnp.concatenate(words, 0)


def finish(parts, visited):
    return pl.pallas_call(
        finish_kernel,
        out_shape=(jax.ShapeDtypeStruct((512, 128), jnp.float32), jax.ShapeDtypeStruct((4, 512), jnp.int32)),
        in_specs=[FULL] * 5,
        out_specs=(FULL, FULL),
        name="finish",
    )(*[pltpu.with_memory_space_constraint(v, VM) for v in (*parts, visited)])


O, M, Q, T = (0, 0), (-1, 0), (1, 0), (0, 1)
H0, H1, ALL = (0, 1), (2, 3), (0, 1, 2, 3)


def tiles(array, start, dx, dy, js):
    return tuple((array, start + n, dx, dy, j) for n, j in enumerate(js))


TWO, TWO_O, UP_O, DOWN_O = (0, 1, False), (0, 1, True), (-1, 0, True), (1, 0, True)
UP, DOWN, OWN, OWN_O = (1, 0, False), (-1, 0, False), (0, 0, False), (0, 0, True)
SOON = (TWO, TWO_O, DOWN_O, UP_O, DOWN)


def level(adjacency, frontier, visited):
    totals = {}

    def work(*jobs):
        used = sorted({t[0] for ts, _ in jobs for t in ts})
        each = tuple(
            (b, tuple((used.index(t[0]),) + t[1:] for t in ts)) for ts, blocks in jobs for b in blocks
        )
        got = mm(ab, [totals.get(b) for b, _ in each], [arrays[n] for n in used], each)
        totals.update(zip([b for b, _ in each], got))

    ft = prep(frontier)
    theirs = swap(ft)
    dx, dy = send(ft, "x"), send(ft, "y")
    ox, oy = send(theirs, "x"), send(theirs, "y")
    ab, seen = split(adjacency, visited)

    bx, by = send(dx, "x"), send(dy, "y")
    pn = swap(jnp.concatenate([ox, oy, dx[0:2], dy[2:4]], 0))
    po = pn[8:12]
    cx = send(jnp.concatenate([dy[2:4], pn[6:8], oy[2:4], po[2:4]], 0), "x")
    cy = send(jnp.concatenate([dx[0:2], pn[0:2], ox[0:2], po[0:2]], 0), "y")
    pb = swap(jnp.concatenate([bx[0:2], by[2:4]], 0))
    ex = send(jnp.concatenate([by[2:4], pb[2:4]], 0), "x")
    ey = send(jnp.concatenate([bx[0:2], pb[0:2]], 0), "y")
    hx, hy = send(cx[:4], "x"), send(cy[:4], "y")
    gx, gy = send(ex[:2], "x"), send(ey[:2], "y")
    pc = swap(jnp.concatenate([cx[4:8], cy[4:8], ex[2:4], ey[2:4]], 0))
    arrays = [ft, dx, pn, dy, bx, by, cx, cy, pc, ex, ey, hx, hy, gx, gy]

    own = tiles(0, 0, O, O, ALL)
    n1, n2 = tiles(1, 0, M, O, ALL), tiles(3, 0, O, M, ALL)
    n3, n4 = tiles(2, 0, Q, O, ALL), tiles(2, 4, O, Q, ALL)
    fa = tiles(4, 0, T, O, ALL) + tiles(5, 0, O, T, ALL)
    fb = tiles(6, 0, M, M, H1) + tiles(6, 2, M, Q, H1) + tiles(7, 0, M, M, H0) + tiles(7, 2, Q, M, H0)
    sd = tiles(8, 0, Q, Q, H1) + tiles(8, 2, Q, M, H1) + tiles(8, 4, Q, Q, H0) + tiles(8, 6, M, Q, H0)
    sd = sd + tiles(9, 0, M, T, H1) + tiles(10, 0, T, M, H0) + tiles(8, 8, Q, T, H1) + tiles(8, 10, T, Q, H0)
    la = tiles(11, 0, T, M, H1) + tiles(11, 2, T, Q, H1) + tiles(12, 0, M, T, H0) + tiles(12, 2, Q, T, H0)
    la = la + tiles(13, 0, T, T, H1) + tiles(14, 0, T, T, H0)
    rest = n1 + n2 + n3 + n4 + fa + fb + sd + la

    work((own + n1, SOON))
    work((n2, SOON))
    work((n3, SOON))
    work((n4 + fa, SOON))
    work((fb, SOON))
    work((own + n1 + n2 + n3 + n4 + fa + fb, (UP,)))
    work((sd, (TWO, TWO_O)))
    work((la, (TWO_O, TWO)))
    work((sd + la, (DOWN_O,)))
    work((sd + la, (DOWN,)))
    work((sd + la, (UP_O,)))
    work((sd + la, (UP,)))
    work((own + rest, (OWN_O,)))
    work((own + rest, (OWN,)))

    hop = send(totals[TWO] + swap(totals[TWO_O]), "z")
    got0 = send(totals[DOWN] + swap(totals[DOWN_O]), "z", True)
    got1 = send(totals[UP] + swap(totals[UP_O]) + hop, "z")
    last = swap(totals[OWN_O])
    return finish([totals[OWN], last, got1, got0], seen)


def solution(mesh):
    placed = (P("col", "row"), P(("row", "col"), None), P(None, ("col", "row")))
    return jax.shard_map(
        level,
        mesh=mesh,
        in_specs=placed,
        out_specs=(P(("col", "row"), None), P(None, ("col", "row"))),
        check_vma=False,
    )
```
